32 devices in a mesh: gx: 16 (over z, y, core), gy: 2 (over x).
Axes of the slice: x: 2, y: 2, z: 4, core: 2. Of those that a mesh axis runs over, the one named last changes fastest.
Arguments:
- grid_field: bfloat16 [2, 256, 64, 512], P(None, 'gx', 'gy'), may hold values from -6 to 6
- spectral_weight: bfloat16 [128, 2, 512, 512], P('gx', None, None, 'gy'), may hold values from -0.1875 to 0.1875
- skip_weight: bfloat16 [512, 512], replicated, may hold values from -0.25 to 0.25
- inner_weight: bfloat16 [1024, 512], replicated, may hold values from -0.25 to 0.25
- outer_weight: bfloat16 [1024, 512], replicated, may hold values from -0.1875 to 0.1875
Outputs:
- layer_out: bfloat16 [2, 256, 64, 512], P(None, 'gx', 'gy')
The draws below stay inside these ranges and needn't reach their ends.
All inputs are finite; a program needn't handle non-finite values.
Results may differ from the reference program's by a relative error of at most 0.0093.
Values may be sent and summed in bfloat16 or wider, within the bound.
No kernel may reach another device: no remote copies, remote signals or barrier semaphores. Data moves between devices by JAX's collectives and lax.ppermute only.
A program may use at most 64 MiB of HBM per device.

```python
import math
import jax
import jax.numpy as jnp
from jax import lax

WIDTH = 512
HIDDEN_SIZE = 1024
KX = 16
KY = 8
BATCH = 2
CX = 16
MODES = 128
NX = 256
NY = 64


def shard_levels(rng, extent, cuts, least, largest):
    loudness, own = 1.0, jax.random.fold_in(rng, 6)
    for axis_at, parts in cuts:
        heights = jnp.exp(jax.random.uniform(jax.random.fold_in(own, axis_at), (parts,), jnp.float32, least / len(cuts), largest / len(cuts)))
        loudness = loudness * jnp.repeat(heights, extent[axis_at] // parts).reshape([-1 if axis == axis_at else 1 for axis in range(len(extent))])
    return loudness


def bell_draw(key, shape, spread, limit, shards=(), kind=jnp.bfloat16):
    entries = jax.random.normal(key, shape, jnp.float32) * spread
    if len(shards) > 0:
        entries = shard_levels(key, shape, shards, -0.22, 0.18) * entries
    return jnp.clip(entries, min=-limit, max=limit).astype(kind)


def setup_inputs(seed: int = 0) -> dict:
    arg_keys = jax.random.split(jax.random.key(seed), 6)
    grid_field = bell_draw(arg_keys[0], (BATCH, NX, NY, WIDTH), 1.0, 6.0, ((1, 16), (2, 2)))
    spectral_weight = bell_draw(arg_keys[1], (MODES, 2, WIDTH, WIDTH), (2 * WIDTH) ** -0.5, 0.1875, ((0, 16), (3, 2)))
    skip_weight = bell_draw(arg_keys[2], (WIDTH, WIDTH), WIDTH ** -0.5, 0.25)
    inner_weight = bell_draw(arg_keys[3], (HIDDEN_SIZE, WIDTH), WIDTH ** -0.5, 0.25)
    outer_weight = bell_draw(arg_keys[4], (HIDDEN_SIZE, WIDTH), HIDDEN_SIZE ** -0.5, 0.1875)
    return dict(grid_field=grid_field, spectral_weight=spectral_weight, skip_weight=skip_weight, inner_weight=inner_weight, outer_weight=outer_weight)


def phase_table(row_ids, col_ids, total_rows, total_cols):
    x_modes = jnp.arange(KX, dtype=jnp.int32)
    y_modes = jnp.arange(KY, dtype=jnp.int32)
    x_phase = (x_modes[:, None] * row_ids[None, :] % total_rows).astype(jnp.float32) / total_rows
    y_phase = (y_modes[:, None] * col_ids[None, :] % total_cols).astype(jnp.float32) / total_cols
    angles = (x_phase[:, None, :, None] + y_phase[None, :, None, :]) * (2.0 * math.pi)
    angles = angles.reshape(KX * KY, row_ids.shape[0] * col_ids.shape[0])
    return jnp.concatenate([jnp.cos(angles), -jnp.sin(angles)], axis=0).astype(jnp.bfloat16)

def reference(grid_field, spectral_weight, skip_weight, inner_weight, outer_weight):
    col_ids = jnp.arange(NY, dtype=jnp.int32)
    block_count = NX // CX

    def forward(running, block_id):
        row_ids = block_id * CX + jnp.arange(CX, dtype=jnp.int32)
        basis = phase_table(row_ids, col_ids, NX, NY).astype(jnp.float32)
        piece = lax.dynamic_slice_in_dim(grid_field, (block_id * CX).astype(jnp.int32), CX, 1)
        piece = piece.reshape(BATCH, CX * NY, WIDTH).astype(jnp.float32)
        return (running + jnp.einsum('kn,bnc->kbc', basis, piece), None)
    summed, _ = lax.scan(forward, jnp.zeros((2 * MODES, BATCH, WIDTH), jnp.float32), jnp.arange(block_count, dtype=jnp.int32))
    spectrum = (summed * (1.0 / math.sqrt(NX * NY))).astype(jnp.bfloat16).reshape(2, MODES, BATCH, WIDTH)
    spec_re = spectrum[0].astype(jnp.float32)
    spec_im = spectrum[1].astype(jnp.float32)
    weight_re = spectral_weight[:, 0].astype(jnp.float32)
    weight_im = spectral_weight[:, 1].astype(jnp.float32)
    mixed_re = jnp.einsum('mbc,mcd->mbd', spec_re, weight_re) - jnp.einsum('mbc,mcd->mbd', spec_im, weight_im)
    mixed_im = jnp.einsum('mbc,mcd->mbd', spec_re, weight_im) + jnp.einsum('mbc,mcd->mbd', spec_im, weight_re)
    mixed_modes = jnp.stack([mixed_re, mixed_im]).astype(jnp.bfloat16).reshape(2 * MODES, BATCH, WIDTH)
    mixed_float = mixed_modes.astype(jnp.float32)
    skip_float = skip_weight.astype(jnp.float32)
    inner_float = inner_weight.astype(jnp.float32)
    outer_float = outer_weight.astype(jnp.float32)

    def backward(block_id):
        row_ids = block_id * CX + jnp.arange(CX, dtype=jnp.int32)
        basis = phase_table(row_ids, col_ids, NX, NY).astype(jnp.float32)
        piece = lax.dynamic_slice_in_dim(grid_field, (block_id * CX).astype(jnp.int32), CX, 1)
        piece = piece.reshape(BATCH, CX * NY, WIDTH).astype(jnp.float32)
        spectral = jnp.einsum('kn,kbc->bnc', basis, mixed_float) * (1.0 / math.sqrt(MODES))
        skip_term = jnp.einsum('bnc,cd->bnd', piece, skip_float)
        active = jax.nn.gelu(spectral + skip_term).astype(jnp.bfloat16)
        hidden = jax.nn.gelu(jnp.einsum('bnc,hc->bnh', active.astype(jnp.float32), inner_float)).astype(jnp.bfloat16)
        feed_forward = jnp.einsum('bnh,hc->bnc', hidden.astype(jnp.float32), outer_float)
        return (active.astype(jnp.float32) + feed_forward).astype(jnp.bfloat16)
    blocks_out = lax.map(backward, jnp.arange(block_count, dtype=jnp.int32))
    blocks_out = blocks_out.reshape(block_count, BATCH, CX, NY, WIDTH)
    return blocks_out.transpose(1, 0, 2, 3, 4).reshape(BATCH, NX, NY, WIDTH)
```

```python
import math

import jax
import jax.numpy as jnp
from jax import lax
from jax.sharding import PartitionSpec as P

KX = 16
KY = 8


def bit_count(size):
    bits = size.bit_length() - 1
    assert 1 << bits == size
    return bits


def bit_groups(bits):
    low = [[bit] for bit in range(min(bits, 2))]
    high = [list(range(bit, min(bit + 2, bits))) for bit in range(2, bits, 2)]
    return low + high


def spread(value, bits):
    return sum(((value >> at) & 1) << bit for at, bit in enumerate(bits))


def block_order(x_devices):
    offsets = [0]
    for group in reversed(bit_groups(bit_count(x_devices))):
        offsets = [spread(digit, group) ^ rest for digit in range(1 << len(group)) for rest in offsets]
    return offsets


def exchange(value, x_mask, y_mask):
    x_devices, y_devices = lax.axis_size("gx"), lax.axis_size("gy")
    pairs = [
        (x * y_devices + y, (x ^ x_mask) * y_devices + (y ^ y_mask))
        for x in range(x_devices)
        for y in range(y_devices)
    ]
    return lax.ppermute(value, ("gx", "gy"), pairs)


def basis_table(modes, row_ids, col_ids, total_rows, total_cols):
    x_phase = ((modes // KY)[:, None] * row_ids[None, :] % total_rows).astype(jnp.float32) / total_rows
    y_phase = ((modes % KY)[:, None] * col_ids[None, :] % total_cols).astype(jnp.float32) / total_cols
    angles = (x_phase[:, :, None] + y_phase[:, None, :]) * (2.0 * math.pi)
    angles = angles.reshape(modes.shape[0], -1)
    return jnp.cos(angles), -jnp.sin(angles)


def local(grid_field, spectral_weight, skip_weight, inner_weight, outer_weight):
    micro_count, row_count, col_count, width_count = grid_field.shape
    x_devices = lax.axis_size("gx")
    y_devices = lax.axis_size("gy")
    total_rows = row_count * x_devices
    total_cols = col_count * y_devices
    mode_count = KX * KY
    own_count = mode_count // x_devices
    x_me, y_me = lax.axis_index("gx"), lax.axis_index("gy")
    row_ids = x_me * row_count + jnp.arange(row_count, dtype=jnp.int32)
    col_ids = y_me * col_count + jnp.arange(col_count, dtype=jnp.int32)
    offsets = jnp.array(block_order(x_devices), jnp.int32)
    modes = ((x_me ^ offsets)[:, None] * own_count + jnp.arange(own_count, dtype=jnp.int32)).reshape(-1)
    cos_table, sin_table = basis_table(modes, row_ids, col_ids, total_rows, total_cols)
    cells = row_count * col_count
    basis = jnp.stack(
        [cos_table.reshape(x_devices, own_count, cells), sin_table.reshape(x_devices, own_count, cells)], axis=1
    )
    basis = basis.reshape(2 * mode_count, cells).astype(jnp.bfloat16)
    flat_rows = grid_field.reshape(micro_count, cells, width_count)
    total = jnp.einsum("kn,bnc->bkc", basis, flat_rows, preferred_element_type=jnp.float32)
    total = total.reshape(micro_count, x_devices, 2 * own_count, width_count)

    for group in bit_groups(bit_count(x_devices)):
        radix = 1 << len(group)
        part = total.shape[1] // radix
        arrived = [
            exchange(total[:, digit * part : (digit + 1) * part].astype(jnp.bfloat16), spread(digit, group), 0)
            for digit in range(1, radix)
        ]
        total = total[:, :part]
        for piece in arrived:
            total = total + piece.astype(jnp.float32)
    total = total[:, 0]
    for bit in range(bit_count(y_devices)):
        total = total + exchange(total.astype(jnp.bfloat16), 0, 1 << bit).astype(jnp.float32)

    spectrum = (total * (1.0 / math.sqrt(total_rows * total_cols))).astype(jnp.bfloat16)
    spectrum = spectrum.reshape(micro_count, 2, own_count, width_count)
    by_re = jnp.einsum(
        "bpmc,mcd->pbmd", spectrum, spectral_weight[:, 0], preferred_element_type=jnp.float32
    )
    by_im = jnp.einsum(
        "bpmc,mcd->pbmd", spectrum, spectral_weight[:, 1], preferred_element_type=jnp.float32
    )
    mixed = jnp.stack([by_re[0] - by_im[1], by_im[0] + by_re[1]], axis=1).astype(jnp.bfloat16)
    part_width = mixed.shape[-1]
    blocks = mixed.reshape(1, 1, micro_count, 2 * own_count, part_width)

    for group in reversed(bit_groups(bit_count(x_devices))):
        digits = [blocks] + [exchange(blocks, spread(digit, group), 0) for digit in range(1, 1 << len(group))]
        blocks = jnp.concatenate(digits, axis=1)
        if group == [1]:
            for bit in range(bit_count(y_devices)):
                blocks = jnp.concatenate([blocks, exchange(blocks, 0, 1 << bit)], axis=0)
    gathered = blocks.reshape(y_devices, x_devices, micro_count, 2 * own_count, part_width)
    gathered = gathered[jnp.arange(y_devices, dtype=jnp.int32) ^ y_me]
    gathered = gathered.transpose(2, 1, 3, 0, 4).reshape(micro_count, 2 * mode_count, width_count)

    spectral = jnp.einsum("kn,bkc->bnc", basis, gathered, preferred_element_type=jnp.float32)
    spectral = spectral * (1.0 / math.sqrt(mode_count))
    skip_term = jnp.einsum("bnc,cd->bnd", flat_rows, skip_weight, preferred_element_type=jnp.float32)
    active = jax.nn.gelu(spectral + skip_term).astype(jnp.bfloat16)
    hidden = jax.nn.gelu(jnp.einsum("bnc,hc->bnh", active, inner_weight, preferred_element_type=jnp.float32))
    hidden = hidden.astype(jnp.bfloat16)
    feed_forward = jnp.einsum("bnh,hc->bnc", hidden, outer_weight, preferred_element_type=jnp.float32)
    layer_out = (active.astype(jnp.float32) + feed_forward).astype(jnp.bfloat16)
    return layer_out.reshape(micro_count, row_count, col_count, width_count)


def solution(mesh):
    in_specs = (P(None, "gx", "gy", None), P("gx", None, None, "gy"), P(), P(), P())
    out_specs = P(None, "gx", "gy", None)
    return jax.shard_map(local, mesh=mesh, in_specs=in_specs, out_specs=out_specs, check_vma=False)
```

```python
import functools
import math

import jax
import jax.numpy as jnp
from jax import lax
from jax.experimental import pallas as pl
from jax.experimental.pallas import tpu as pltpu
from jax.sharding import PartitionSpec as P


KX = 16
KY = 8
VMEM = pl.BlockSpec(memory_space=pltpu.VMEM)


def hops(mask, low_bits):
    low, high = mask & ((1 << low_bits) - 1), mask >> low_bits
    return low.bit_count() + (high + high.bit_count()) / 2


def share(masks, low_bits):
    order = sorted(masks, key=lambda mask: -hops(mask, low_bits))
    pairs = [(order[at], order[at + 1]) for at in range(0, len(order) - 1, 2)]
    return pairs, order[-1]


def exchange(value, x_masks, y_mask):
    x_devices, y_devices = lax.axis_size("gx"), lax.axis_size("gy")
    pairs = [
        (x * y_devices + y, (x ^ x_masks[x & 1]) * y_devices + (y ^ y_mask))
        for x in range(x_devices)
        for y in range(y_devices)
    ]
    return lax.ppermute(value, ("gx", "gy"), pairs)


def reduce_offsets(x_devices):
    pairs, shared = share(range(1, x_devices // 2), 1)
    keep = []
    for core in (0, 1):
        blocks = [2 * pair[core] + kind for pair in pairs for kind in (0, 1)]
        keep.append(blocks + [2 * shared, 0])
    return [keep[core] + [offset ^ 1 for offset in keep[1 - core]] for core in (0, 1)]


def gather_offsets(x_devices):
    held = [4 * mask for mask in range(x_devices // 4)]
    blocks = [holder ^ (2 * y) ^ offset for holder in (0, 1) for y in (0, 1) for offset in held]
    return [blocks, blocks]


def divide(value, by):
    return value >> (by.bit_length() - 1) if by & (by - 1) == 0 else value // by


def remainder(value, by):
    return value & (by - 1) if by & (by - 1) == 0 else value % by


def write_basis(offsets, own_count, shape, x_wave, y_wave, basis):
    row_count, col_count, total_rows, total_cols = shape
    cells = row_count * col_count
    x_me, y_me = lax.axis_index("gx"), lax.axis_index("gy")
    x_at = divide(lax.broadcasted_iota(jnp.int32, (KX, cells), 1), col_count) + x_me * row_count
    x_turn = remainder(lax.broadcasted_iota(jnp.int32, (KX, cells), 0) * x_at, total_rows)
    x_angle = x_turn.astype(jnp.float32) * (2.0 * math.pi / total_rows)
    x_wave[0], x_wave[1] = jnp.cos(x_angle), jnp.sin(x_angle)
    y_at = remainder(lax.broadcasted_iota(jnp.int32, (KY, cells), 1), col_count) + y_me * col_count
    y_turn = remainder(lax.broadcasted_iota(jnp.int32, (KY, cells), 0) * y_at, total_cols)
    y_angle = y_turn.astype(jnp.float32) * (2.0 * math.pi / total_cols)
    y_wave[0], y_wave[1] = jnp.cos(y_angle), jnp.sin(y_angle)
    run = min(own_count, KY)
    core = x_me & 1
    pending, row = [], 0
    for at in range(len(offsets[0])):
        owner = x_me ^ jnp.where(core == 0, offsets[0][at], offsets[1][at])
        cosines, sines = [], []
        for start in range(0, own_count, run):
            mode = owner * own_count + start
            x_mode = mode // KY
            x_cos, x_sin = x_wave[0, pl.ds(x_mode, 1), :], x_wave[1, pl.ds(x_mode, 1), :]
            if run == KY:
                y_cos, y_sin = y_wave[0], y_wave[1]
            else:
                y_cos, y_sin = y_wave[0, :run], y_wave[1, :run]
                for other in range(run, KY, run):
                    here = mode % KY == other
                    y_cos = jnp.where(here, y_wave[0, other : other + run], y_cos)
                    y_sin = jnp.where(here, y_wave[1, other : other + run], y_sin)
            cosines.append(x_cos * y_cos - x_sin * y_sin)
            sines.append(-(x_sin * y_cos + x_cos * y_sin))
        pending += cosines + sines
        count = sum(piece.shape[0] for piece in pending)
        if count % 16 == 0:
            basis[row : row + count, :] = jnp.concatenate(pending, axis=0).astype(jnp.bfloat16)
            pending, row = [], row + count


def basis_kernel(offsets, own_count, shape, basis, x_wave, y_wave):
    write_basis(offsets, own_count, shape, x_wave, y_wave, basis)


def forward_kernel(basis, field, keep, send):
    half = basis.shape[0] // 2
    for b in range(field.shape[0]):
        send[b] = jnp.dot(basis[half:, :], field[b], preferred_element_type=jnp.float32).astype(jnp.bfloat16)
        keep[b] = jnp.dot(basis[:half, :], field[b], preferred_element_type=jnp.float32)


def skip_kernel(offsets, own_count, shape, field, skip_weight, skip, turned, x_wave, y_wave, basis):
    for b in range(field.shape[0]):
        skip[b] = jnp.dot(field[b], skip_weight[...], preferred_element_type=jnp.float32)
    write_basis(offsets, own_count, shape, x_wave, y_wave, basis)
    turned[...] = basis[...].T


def mix_kernel(scale, own_count, total, other, weight, mixed):
    micro_count, rows, width_count = total.shape
    spectrum = ((total[...] + other[...].astype(jnp.float32)) * scale).reshape(micro_count * rows, width_count)
    mode = remainder(lax.broadcasted_iota(jnp.int32, spectrum.shape, 0), own_count)
    apart = [jnp.where(mode == at, spectrum, 0.0).astype(jnp.bfloat16) for at in range(own_count)]
    apart = jnp.concatenate(apart, axis=1)
    part_width = mixed.shape[-1]
    by = []
    for kind in (0, 1):
        columns = weight[:, kind].reshape(own_count * width_count, part_width)
        product = jnp.dot(apart, columns, preferred_element_type=jnp.float32)
        by.append(product.reshape(micro_count, rows, part_width))
    real = by[0][:, :own_count] - by[1][:, own_count:]
    imaginary = by[1][:, :own_count] + by[0][:, own_count:]
    mixed[...] = jnp.concatenate([real, imaginary], axis=1).astype(jnp.bfloat16)


def gelu(value):
    inner = value * (math.sqrt(2.0 / math.pi) + (math.sqrt(2.0 / math.pi) * 0.044715) * (value * value))
    half = 0.5 * value
    return half + half * jnp.tanh(inner)


def output_kernel(
    scale, tile, chunk, y_devices, mine, theirs, skip, turned, inner_weight, outer_weight, out, modes
):
    micro_count, cells, _ = skip.shape
    step = pl.program_id(0)
    tiles = cells // tile

    @pl.when(step == 0)
    def _():
        y_me = lax.axis_index("gy") if y_devices > 1 else 0
        planes, held_count, _, rows, part_width = mine.shape
        row = 0
        for source in (mine, theirs):
            for y in range(planes // y_devices):
                for part in range(y_devices):
                    plane = y * y_devices + (y_me ^ part)
                    for at in range(held_count):
                        for b in range(micro_count):
                            modes[b, row + at * rows : row + (at + 1) * rows, part * part_width : (part + 1) * part_width] = (
                                source[plane, at, b]
                            )
                row += held_count * rows

    b, start = step // tiles, pl.multiple_of((step % tiles) * tile, tile)
    spectral = jnp.dot(turned[pl.ds(start, tile), :], modes[b], preferred_element_type=jnp.float32)
    active = gelu(spectral * scale + skip[b, pl.ds(start, tile), :]).astype(jnp.bfloat16)

    def inner(at):
        columns = inner_weight[at * chunk : (at + 1) * chunk, :]
        return lax.dot_general(active, columns, (((1,), (1,)), ((), ())), preferred_element_type=jnp.float32)

    chunks = inner_weight.shape[0] // chunk
    total, following = active.astype(jnp.float32), inner(0)
    for at in range(chunks):
        hidden = following
        if at + 1 < chunks:
            following = inner(at + 1)
        rows = outer_weight[at * chunk : (at + 1) * chunk, :]
        total = total + jnp.dot(gelu(hidden).astype(jnp.bfloat16), rows, preferred_element_type=jnp.float32)
    out[0] = total.astype(jnp.bfloat16)


def local(grid_field, spectral_weight, skip_weight, inner_weight, outer_weight):
    micro_count, row_count, col_count, width_count = grid_field.shape
    x_devices = lax.axis_size("gx")
    y_devices = lax.axis_size("gy")
    total_rows = row_count * x_devices
    total_cols = col_count * y_devices
    mode_count = KX * KY
    own_count = mode_count // x_devices
    cells = row_count * col_count
    shape = (row_count, col_count, total_rows, total_cols)
    flat_rows = grid_field.reshape(micro_count, cells, width_count)
    waves = [pltpu.VMEM((2, KX, cells), jnp.float32), pltpu.VMEM((2, KY, cells), jnp.float32)]
    basis_shape = (2 * mode_count, cells)
    matmul = 2 * micro_count * cells * width_count

    basis = pl.pallas_call(
        functools.partial(basis_kernel, reduce_offsets(x_devices), own_count, shape),
        out_shape=jax.ShapeDtypeStruct(basis_shape, jnp.bfloat16),
        out_specs=VMEM,
        scratch_shapes=waves,
        compiler_params=pltpu.CompilerParams(vmem_limit_bytes=16 * 2**20),
        cost_estimate=pl.CostEstimate(flops=8 * matmul * 2 * mode_count, bytes_accessed=2 * flat_rows.size, transcendentals=0),
        name="basis",
    )()
    keep, send = pl.pallas_call(
        forward_kernel,
        out_shape=[
            jax.ShapeDtypeStruct((micro_count, mode_count, width_count), jnp.float32),
            jax.ShapeDtypeStruct((micro_count, mode_count, width_count), jnp.bfloat16),
        ],
        in_specs=[VMEM, VMEM],
        out_specs=[VMEM, VMEM],
        compiler_params=pltpu.CompilerParams(vmem_limit_bytes=16 * 2**20),
        cost_estimate=pl.CostEstimate(flops=8 * matmul * 2 * mode_count, bytes_accessed=2 * flat_rows.size, transcendentals=0),
        name="forward",
    )(basis, flat_rows)

    skip, turned = pl.pallas_call(
        functools.partial(skip_kernel, gather_offsets(x_devices), own_count, shape),
        out_shape=[
            jax.ShapeDtypeStruct((micro_count, cells, width_count), jnp.float32),
            jax.ShapeDtypeStruct((cells, 2 * mode_count), jnp.bfloat16),
        ],
        in_specs=[VMEM, VMEM],
        out_specs=[VMEM, VMEM],
        scratch_shapes=waves + [pltpu.VMEM(basis_shape, jnp.bfloat16)],
        compiler_params=pltpu.CompilerParams(vmem_limit_bytes=16 * 2**20),
        cost_estimate=pl.CostEstimate(flops=matmul * width_count, bytes_accessed=2 * flat_rows.size, transcendentals=0),
        name="skip",
    )(flat_rows, skip_weight)

    def as_blocks(array):
        return array.reshape(micro_count, x_devices // 2, 2 * own_count, width_count)

    pairs, shared = share(range(1, x_devices // 2), 1)
    blocks = as_blocks(keep) + as_blocks(exchange(send, (1, 1), 0)).astype(jnp.float32)
    arrived = [
        exchange(blocks[:, 2 * at : 2 * at + 2].astype(jnp.bfloat16), (2 * pair[0], 2 * pair[1]), 0)
        for at, pair in enumerate(pairs)
    ]
    shared_arrived = exchange(blocks[:, -2].astype(jnp.bfloat16), (2 * shared, 2 * shared), 0)
    summed = sum(piece.astype(jnp.float32) for piece in arrived)
    swapped = exchange(summed[:, 1].astype(jnp.bfloat16), (1, 1), 0)
    total = blocks[:, -1] + summed[:, 0] + shared_arrived.astype(jnp.float32) + swapped.astype(jnp.float32)
    for bit in range(y_devices.bit_length() - 1):
        if bit > 0:
            total = total + other.astype(jnp.float32)
        other = exchange(total.astype(jnp.bfloat16), (0, 0), 1 << bit)

    part_width = spectral_weight.shape[-1]
    mixed = pl.pallas_call(
        functools.partial(mix_kernel, 1.0 / math.sqrt(total_rows * total_cols), own_count),
        out_shape=jax.ShapeDtypeStruct((micro_count, 2 * own_count, part_width), jnp.bfloat16),
        in_specs=[VMEM] * 3,
        out_specs=VMEM,
        compiler_params=pltpu.CompilerParams(vmem_limit_bytes=16 * 2**20),
        cost_estimate=pl.CostEstimate(flops=8 * spectral_weight.size, bytes_accessed=2 * spectral_weight.size, transcendentals=0),
        name="mix",
    )(total, other, spectral_weight)[None]

    pairs, shared = share(range(1, x_devices // 4), 0)
    along = []
    for mask in range(1, x_devices // 4):
        along.append(exchange(mixed, (4 * mask, 4 * mask), 0))
    held = jnp.concatenate([mixed] + along, axis=0)
    plane = [(y, part) for y in (0, 1) for part in range(y_devices)]
    mine = jnp.stack([held] + [exchange(held, (2 * y, 2 * y), part) for y, part in plane[1:]])
    theirs = exchange(mine, (1, 1), 0)

    rows = 2 * own_count
    if rows % 16 or part_width % 128:
        whole = jnp.stack([mine, theirs]).reshape((2, 2, y_devices) + mine.shape[1:])
        whole = jnp.take(whole, lax.axis_index("gy") ^ jnp.arange(y_devices, dtype=jnp.int32), axis=2)
        whole = whole.transpose(0, 1, 4, 3, 5, 2, 6).reshape(2, 2, 1, micro_count, -1, width_count)
        mine, theirs = whole[0], whole[1]
        parts = 1
    else:
        parts = y_devices
    tile = cells
    layer_out = pl.pallas_call(
        functools.partial(output_kernel, 1.0 / math.sqrt(mode_count), tile, inner_weight.shape[0] // 2, parts),
        out_shape=jax.ShapeDtypeStruct((micro_count, cells, width_count), jnp.bfloat16),
        grid=(micro_count * cells // tile,),
        in_specs=[VMEM] * 6,
        out_specs=pl.BlockSpec((1, tile, width_count), lambda i: (i // (cells // tile), i % (cells // tile), 0)),
        scratch_shapes=[
            pltpu.VMEM((micro_count, 2 * mode_count, width_count), jnp.bfloat16),
        ],
        compiler_params=pltpu.CompilerParams(vmem_limit_bytes=32 * 2**20),
        cost_estimate=pl.CostEstimate(
            flops=matmul * (2 * mode_count + 2 * inner_weight.shape[0]), bytes_accessed=4 * flat_rows.size, transcendentals=0
        ),
        name="output",
    )(mine, theirs, skip, turned, inner_weight, outer_weight)
    return layer_out.reshape(micro_count, row_count, col_count, width_count)


def solution(mesh):
    in_specs = (P(None, "gx", "gy", None), P("gx", None, None, "gy"), P(), P(), P())
    out_specs = P(None, "gx", "gy", None)
    return jax.shard_map(local, mesh=mesh, in_specs=in_specs, out_specs=out_specs, check_vma=False)
```

```python
import functools
import math

import jax
import jax.numpy as jnp
from jax import lax
from jax.experimental import pallas as pl
from jax.experimental.pallas import tpu as pltpu
from jax.sharding import PartitionSpec as P


KX = 16
KY = 8
VMEM = pl.BlockSpec(memory_space=pltpu.VMEM)


def reduce_peers(chips):
    even, odd = list(range(chips - 2, 0, -2)), list(range(chips - 1, 1, -2))
    if not even:
        return [], 1
    return list(zip(even[1:] + [1], odd)), even[0]


def gather_peers(masks):
    masks = list(masks)
    return [(masks[at], masks[at + 1]) for at in range(0, len(masks) - 1, 2)], masks[-1]


def along_peers(places):
    middle = places // 2
    return gather_peers([mask for mask in range(1, places) if mask != middle] + [middle])


def plane_peers(y_devices):
    return gather_peers([(y, part) for y in (0, 1) for part in range(y_devices) if y or part])


def exchange(value, x_masks, y_masks=(0, 0)):
    x_devices, y_devices = lax.axis_size("gx"), lax.axis_size("gy")
    pairs = [
        (x * y_devices + y, (x ^ x_masks[x & 1]) * y_devices + (y ^ y_masks[x & 1]))
        for x in range(x_devices)
        for y in range(y_devices)
    ]
    return lax.ppermute(value, ("gx", "gy"), pairs)


def reduce_offsets(x_devices):
    pairs, shared = reduce_peers(x_devices // 2)
    keep = []
    for core in (0, 1):
        blocks = [2 * pair[core] + kind for pair in pairs for kind in (0, 1)]
        keep.append(blocks + [2 * shared, 0])
    return [keep[core] + [offset ^ 1 for offset in keep[1 - core]] for core in (0, 1)]


def gather_offsets(x_devices):
    pairs, shared = along_peers(x_devices // 4)
    held = []
    for core in (0, 1):
        held.append([0, 4 * shared] + [4 * pair[core] + kind for pair in pairs for kind in (0, 1)])
    return [
        [holder ^ (2 * y) ^ offset for holder in (0, 1) for y in (0, 1) for offset in held[core ^ holder]]
        for core in (0, 1)
    ]


def find_blocks(y_devices, core, chip, mine, theirs):
    pairs, shared = plane_peers(y_devices)
    blocks = {(holder, 0, 0): chip(holder) for holder in (0, 1)}
    blocks[0, *shared], blocks[1, *shared] = mine(0), theirs(0)
    for at, pair in enumerate(pairs):
        for server in (0, 1):
            for holder in (0, 1):
                ours, other = mine(1 + 2 * at + holder), theirs(1 + 2 * at + (1 - holder))
                blocks[holder, *pair[server]] = jnp.where(core == server, ours, other)
    return blocks


def divide(value, by):
    return value >> (by.bit_length() - 1) if by & (by - 1) == 0 else value // by


def remainder(value, by):
    return value & (by - 1) if by & (by - 1) == 0 else value % by


def write_basis(offsets, own_count, shape, x_wave, y_wave, basis):
    row_count, col_count, total_rows, total_cols = shape
    cells = row_count * col_count
    x_me, y_me = lax.axis_index("gx"), lax.axis_index("gy")
    x_at = divide(lax.broadcasted_iota(jnp.int32, (KX, cells), 1), col_count) + x_me * row_count
    x_turn = remainder(lax.broadcasted_iota(jnp.int32, (KX, cells), 0) * x_at, total_rows)
    x_angle = x_turn.astype(jnp.float32) * (2.0 * math.pi / total_rows)
    x_wave[0], x_wave[1] = jnp.cos(x_angle), jnp.sin(x_angle)
    y_at = remainder(lax.broadcasted_iota(jnp.int32, (KY, cells), 1), col_count) + y_me * col_count
    y_turn = remainder(lax.broadcasted_iota(jnp.int32, (KY, cells), 0) * y_at, total_cols)
    y_angle = y_turn.astype(jnp.float32) * (2.0 * math.pi / total_cols)
    y_wave[0], y_wave[1] = jnp.cos(y_angle), jnp.sin(y_angle)
    run = min(own_count, KY)
    core = x_me & 1
    pending, row = [], 0
    for at in range(len(offsets[0])):
        owner = x_me ^ jnp.where(core == 0, offsets[0][at], offsets[1][at])
        cosines, sines = [], []
        for start in range(0, own_count, run):
            mode = owner * own_count + start
            x_mode = mode // KY
            x_cos, x_sin = x_wave[0, pl.ds(x_mode, 1), :], x_wave[1, pl.ds(x_mode, 1), :]
            if run == KY:
                y_cos, y_sin = y_wave[0], y_wave[1]
            else:
                y_cos, y_sin = y_wave[0, :run], y_wave[1, :run]
                for other in range(run, KY, run):
                    here = mode % KY == other
                    y_cos = jnp.where(here, y_wave[0, other : other + run], y_cos)
                    y_sin = jnp.where(here, y_wave[1, other : other + run], y_sin)
            cosines.append(x_cos * y_cos - x_sin * y_sin)
            sines.append(-(x_sin * y_cos + x_cos * y_sin))
        pending += cosines + sines
        count = sum(piece.shape[0] for piece in pending)
        if count % 16 == 0:
            basis[row : row + count, :] = jnp.concatenate(pending, axis=0).astype(jnp.bfloat16)
            pending, row = [], row + count


def basis_kernel(offsets, own_count, shape, basis, x_wave, y_wave):
    write_basis(offsets, own_count, shape, x_wave, y_wave, basis)


def forward_kernel(half, basis, field, out):
    rows = out.shape[1]
    for b in range(field.shape[0]):
        product = jnp.dot(basis[half * rows : (half + 1) * rows, :], field[b], preferred_element_type=jnp.float32)
        out[b] = product.astype(out.dtype)


def skip_kernel(offsets, own_count, shape, field, skip_weight, skip, turned, x_wave, y_wave, basis):
    for b in range(field.shape[0]):
        skip[b] = jnp.dot(field[b], skip_weight[...], preferred_element_type=jnp.float32)
    write_basis(offsets, own_count, shape, x_wave, y_wave, basis)
    turned[...] = basis[...].T


def mix_kernel(scale, own_count, total, other, weight, mixed):
    micro_count, rows, width_count = total.shape
    spectrum = ((total[...] + other[...].astype(jnp.float32)) * scale).reshape(micro_count * rows, width_count)
    mode = remainder(lax.broadcasted_iota(jnp.int32, spectrum.shape, 0), own_count)
    apart = [jnp.where(mode == at, spectrum, 0.0).astype(jnp.bfloat16) for at in range(own_count)]
    apart = jnp.concatenate(apart, axis=1)
    part_width = mixed.shape[-1]
    by = []
    for kind in (0, 1):
        columns = weight[:, kind].reshape(own_count * width_count, part_width)
        product = jnp.dot(apart, columns, preferred_element_type=jnp.float32)
        by.append(product.reshape(micro_count, rows, part_width))
    real = by[0][:, :own_count] - by[1][:, own_count:]
    imaginary = by[1][:, :own_count] + by[0][:, own_count:]
    mixed[...] = jnp.concatenate([real, imaginary], axis=1).astype(jnp.bfloat16)


def gelu(value):
    inner = value * (math.sqrt(2.0 / math.pi) + (math.sqrt(2.0 / math.pi) * 0.044715) * (value * value))
    half = 0.5 * value
    return half + half * jnp.tanh(inner)


def output_kernel(
    scale, tile, chunk, y_devices, chip, mine, theirs, skip, turned, inner_weight, outer_weight, out, modes
):
    micro_count, cells, _ = skip.shape
    step = pl.program_id(0)
    tiles = cells // tile

    @pl.when(step == 0)
    def _():
        if y_devices == 1:
            count = chip.shape[2]
            for at in range(chip.shape[0]):
                for b in range(micro_count):
                    modes[b, 0, at * count : (at + 1) * count, :] = chip[at, b]
            return
        core, y_me = lax.axis_index("gx") & 1, lax.axis_index("gy")
        _, held_count, _, rows, part_width = chip.shape
        count = held_count * rows
        for b in range(micro_count):
            found = find_blocks(
                y_devices, core, lambda i: chip[i, :, b], lambda i: mine[i, :, b], lambda i: theirs[i, :, b]
            )
            for (holder, y, part), blocks in found.items():
                at = (2 * holder + y) * count
                modes[b, y_me ^ part, at : at + count, :] = blocks.reshape(count, part_width)

    b, start = step // tiles, pl.multiple_of((step % tiles) * tile, tile)
    waves = turned[pl.ds(start, tile), :]
    spectral = jnp.concatenate(
        [jnp.dot(waves, modes[b, part], preferred_element_type=jnp.float32) for part in range(modes.shape[1])], axis=1
    )
    active = gelu(spectral * scale + skip[b, pl.ds(start, tile), :]).astype(jnp.bfloat16)

    def inner(at):
        columns = inner_weight[at * chunk : (at + 1) * chunk, :]
        return lax.dot_general(active, columns, (((1,), (1,)), ((), ())), preferred_element_type=jnp.float32)

    chunks = inner_weight.shape[0] // chunk
    total, following = active.astype(jnp.float32), inner(0)
    for at in range(chunks):
        hidden = following
        if at + 1 < chunks:
            following = inner(at + 1)
        rows = outer_weight[at * chunk : (at + 1) * chunk, :]
        total = total + jnp.dot(gelu(hidden).astype(jnp.bfloat16), rows, preferred_element_type=jnp.float32)
    out[0] = total.astype(jnp.bfloat16)


def local(grid_field, spectral_weight, skip_weight, inner_weight, outer_weight):
    micro_count, row_count, col_count, width_count = grid_field.shape
    x_devices = lax.axis_size("gx")
    y_devices = lax.axis_size("gy")
    total_rows = row_count * x_devices
    total_cols = col_count * y_devices
    mode_count = KX * KY
    own_count = mode_count // x_devices
    cells = row_count * col_count
    shape = (row_count, col_count, total_rows, total_cols)
    flat_rows = grid_field.reshape(micro_count, cells, width_count)
    waves = [pltpu.VMEM((2, KX, cells), jnp.float32), pltpu.VMEM((2, KY, cells), jnp.float32)]
    basis_shape = (2 * mode_count, cells)
    matmul = 2 * micro_count * cells * width_count

    basis = pl.pallas_call(
        functools.partial(basis_kernel, reduce_offsets(x_devices), own_count, shape),
        out_shape=jax.ShapeDtypeStruct(basis_shape, jnp.bfloat16),
        out_specs=VMEM,
        scratch_shapes=waves,
        compiler_params=pltpu.CompilerParams(vmem_limit_bytes=16 * 2**20),
        cost_estimate=pl.CostEstimate(flops=8 * matmul * 2 * mode_count, bytes_accessed=2 * flat_rows.size, transcendentals=0),
        name="basis",
    )()

    def forward(half, kind):
        return pl.pallas_call(
            functools.partial(forward_kernel, half),
            out_shape=jax.ShapeDtypeStruct((micro_count, mode_count, width_count), kind),
            in_specs=[VMEM, VMEM],
            out_specs=VMEM,
            compiler_params=pltpu.CompilerParams(vmem_limit_bytes=16 * 2**20),
            cost_estimate=pl.CostEstimate(
                flops=8 * matmul * mode_count, bytes_accessed=2 * flat_rows.size, transcendentals=0
            ),
            name="forward",
        )(basis, flat_rows)

    send = forward(1, jnp.bfloat16)
    keep = forward(0, jnp.float32)

    skip, turned = pl.pallas_call(
        functools.partial(skip_kernel, gather_offsets(x_devices), own_count, shape),
        out_shape=[
            jax.ShapeDtypeStruct((micro_count, cells, width_count), jnp.float32),
            jax.ShapeDtypeStruct((cells, 2 * mode_count), jnp.bfloat16),
        ],
        in_specs=[VMEM, VMEM],
        out_specs=[VMEM, VMEM],
        scratch_shapes=waves + [pltpu.VMEM(basis_shape, jnp.bfloat16)],
        compiler_params=pltpu.CompilerParams(vmem_limit_bytes=16 * 2**20),
        cost_estimate=pl.CostEstimate(flops=matmul * width_count, bytes_accessed=2 * flat_rows.size, transcendentals=0),
        name="skip",
    )(flat_rows, skip_weight)

    def as_blocks(array):
        return array.reshape(micro_count, x_devices // 2, 2 * own_count, width_count)

    pairs, shared = reduce_peers(x_devices // 2)
    sent = exchange(send, (1, 1))
    blocks = as_blocks(keep) + as_blocks(sent).astype(jnp.float32)
    arrived = []
    for at, pair in enumerate(pairs):
        arrived.append(exchange(blocks[:, 2 * at : 2 * at + 2].astype(jnp.bfloat16), (2 * pair[0], 2 * pair[1])))
    shared_arrived = exchange(blocks[:, -2].astype(jnp.bfloat16), (2 * shared, 2 * shared))
    summed = sum(piece.astype(jnp.float32) for piece in arrived)
    swapped = exchange(summed[:, 1].astype(jnp.bfloat16), (1, 1))
    total = blocks[:, -1] + summed[:, 0] + shared_arrived.astype(jnp.float32) + swapped.astype(jnp.float32)
    for bit in range(y_devices.bit_length() - 1):
        if bit > 0:
            total = total + other.astype(jnp.float32)
        other = exchange(total.astype(jnp.bfloat16), (0, 0), (1 << bit, 1 << bit))

    part_width = spectral_weight.shape[-1]
    mixed = pl.pallas_call(
        functools.partial(mix_kernel, 1.0 / math.sqrt(total_rows * total_cols), own_count),
        out_shape=jax.ShapeDtypeStruct((micro_count, 2 * own_count, part_width), jnp.bfloat16),
        in_specs=[VMEM] * 3,
        out_specs=VMEM,
        compiler_params=pltpu.CompilerParams(vmem_limit_bytes=16 * 2**20),
        cost_estimate=pl.CostEstimate(flops=8 * spectral_weight.size, bytes_accessed=2 * spectral_weight.size, transcendentals=0),
        name="mix",
    )(total, other, spectral_weight)[None]

    pairs, shared = along_peers(x_devices // 4)
    sibling = exchange(mixed, (1, 1))
    shared_along = exchange(mixed, (4 * shared, 4 * shared))
    chip = jnp.concatenate([mixed, sibling])
    along = []
    for pair in pairs:
        along.append(exchange(chip, (4 * pair[0], 4 * pair[1])))
    held = jnp.concatenate([mixed, shared_along] + along)

    pairs, shared = plane_peers(y_devices)
    sibling = exchange(held, (1, 1))
    shared_plane = exchange(held, (2 * shared[0], 2 * shared[0]), (shared[1], shared[1]))
    chip = jnp.stack([held, sibling])
    planes = []
    for one, two in pairs:
        planes.append(exchange(chip, (2 * one[0], 2 * two[0]), (one[1], two[1])))
    mine = jnp.concatenate([shared_plane[None]] + planes)
    theirs = exchange(mine, (1, 1))

    rows = 2 * own_count
    parts = y_devices
    if rows % 16 or part_width % 128:
        core = lax.axis_index("gx") & 1
        found = find_blocks(y_devices, core, lambda i: chip[i], lambda i: mine[i], lambda i: theirs[i])
        whole = jnp.stack([jnp.stack([found[h, y, p] for p in range(y_devices)]) for h in (0, 1) for y in (0, 1)])
        whole = jnp.take(whole, lax.axis_index("gy") ^ jnp.arange(y_devices, dtype=jnp.int32), axis=1)
        chip = whole.transpose(0, 3, 2, 4, 1, 5).reshape(4, micro_count, -1, width_count)
        parts, mine, theirs = 1, chip[:, :1, :16], chip[:, :1, :16]
    tile = cells
    layer_out = pl.pallas_call(
        functools.partial(output_kernel, 1.0 / math.sqrt(mode_count), tile, inner_weight.shape[0] // 2, parts),
        out_shape=jax.ShapeDtypeStruct((micro_count, cells, width_count), jnp.bfloat16),
        grid=(micro_count * cells // tile,),
        in_specs=[VMEM] * 7,
        out_specs=pl.BlockSpec((1, tile, width_count), lambda i: (i // (cells // tile), i % (cells // tile), 0)),
        scratch_shapes=[
            pltpu.VMEM((micro_count, parts, 2 * mode_count, width_count // parts), jnp.bfloat16),
        ],
        compiler_params=pltpu.CompilerParams(vmem_limit_bytes=32 * 2**20),
        cost_estimate=pl.CostEstimate(
            flops=matmul * (2 * mode_count + 2 * inner_weight.shape[0]), bytes_accessed=4 * flat_rows.size, transcendentals=0
        ),
        name="output",
    )(chip, mine, theirs, skip, turned, inner_weight, outer_weight)
    return layer_out.reshape(micro_count, row_count, col_count, width_count)


def solution(mesh):
    in_specs = (P(None, "gx", "gy", None), P("gx", None, None, "gy"), P(), P(), P())
    out_specs = P(None, "gx", "gy", None)
    return jax.shard_map(local, mesh=mesh, in_specs=in_specs, out_specs=out_specs, check_vma=False)
```

```python
import functools
import math

import jax
import jax.numpy as jnp
from jax import lax
from jax.experimental import pallas as pl
from jax.experimental.pallas import tpu as pltpu
from jax.sharding import PartitionSpec as P


KX = 16
KY = 8
VMEM = pl.BlockSpec(memory_space=pltpu.VMEM)


def reduce_peers(chips):
    even, odd = list(range(chips - 2, 0, -2)), list(range(chips - 1, 1, -2))
    if not even:
        return [], 1
    return list(zip(even[1:] + [1], odd)), even[0]


def gather_peers(masks):
    masks = list(masks)
    return [(masks[at], masks[at + 1]) for at in range(0, len(masks) - 1, 2)], masks[-1]


def along_peers(places):
    middle = places // 2
    return gather_peers([mask for mask in range(1, places) if mask != middle] + [middle])


def plane_peers(y_devices):
    return gather_peers([(y, part) for y in (0, 1) for part in range(y_devices) if y or part])


def exchange(value, x_masks, y_masks=(0, 0)):
    x_devices, y_devices = lax.axis_size("gx"), lax.axis_size("gy")
    pairs = [
        (x * y_devices + y, (x ^ x_masks[x & 1]) * y_devices + (y ^ y_masks[x & 1]))
        for x in range(x_devices)
        for y in range(y_devices)
    ]
    return lax.ppermute(value, ("gx", "gy"), pairs)


def reduce_offsets(x_devices):
    pairs, shared = reduce_peers(x_devices // 2)
    keep = []
    for core in (0, 1):
        blocks = [2 * pair[core] + kind for pair in pairs for kind in (0, 1)]
        keep.append(blocks + [2 * shared, 0])
    return [keep[core] + [offset ^ 1 for offset in keep[1 - core]] for core in (0, 1)]


def gather_offsets(x_devices):
    pairs, shared = along_peers(x_devices // 4)
    held = []
    for core in (0, 1):
        held.append([0, 4 * shared] + [4 * pair[core] + kind for pair in pairs for kind in (0, 1)])
    return [
        [holder ^ (2 * y) ^ offset for holder in (0, 1) for y in (0, 1) for offset in held[core ^ holder]]
        for core in (0, 1)
    ]


def find_blocks(y_devices, core, chip, mine, theirs):
    pairs, shared = plane_peers(y_devices)
    blocks = {(holder, 0, 0): chip(holder) for holder in (0, 1)}
    blocks[0, *shared], blocks[1, *shared] = mine(0), theirs(0)
    for at, pair in enumerate(pairs):
        for server in (0, 1):
            for holder in (0, 1):
                ours, other = mine(1 + 2 * at + holder), theirs(1 + 2 * at + (1 - holder))
                blocks[holder, *pair[server]] = jnp.where(core == server, ours, other)
    return blocks


def divide(value, by):
    return value >> (by.bit_length() - 1) if by & (by - 1) == 0 else value // by


def remainder(value, by):
    return value & (by - 1) if by & (by - 1) == 0 else value % by


def write_basis(offsets, own_count, shape, x_wave, y_wave, basis):
    row_count, col_count, total_rows, total_cols = shape
    cells = row_count * col_count
    x_me, y_me = lax.axis_index("gx"), lax.axis_index("gy")
    x_at = divide(lax.broadcasted_iota(jnp.int32, (KX, cells), 1), col_count) + x_me * row_count
    x_turn = remainder(lax.broadcasted_iota(jnp.int32, (KX, cells), 0) * x_at, total_rows)
    x_angle = x_turn.astype(jnp.float32) * (2.0 * math.pi / total_rows)
    x_wave[0], x_wave[1] = jnp.cos(x_angle), jnp.sin(x_angle)
    y_at = remainder(lax.broadcasted_iota(jnp.int32, (KY, cells), 1), col_count) + y_me * col_count
    y_turn = remainder(lax.broadcasted_iota(jnp.int32, (KY, cells), 0) * y_at, total_cols)
    y_angle = y_turn.astype(jnp.float32) * (2.0 * math.pi / total_cols)
    y_wave[0], y_wave[1] = jnp.cos(y_angle), jnp.sin(y_angle)
    run = min(own_count, KY)
    core = x_me & 1
    pending, row = [], 0
    for at in range(len(offsets[0])):
        owner = x_me ^ jnp.where(core == 0, offsets[0][at], offsets[1][at])
        cosines, sines = [], []
        for start in range(0, own_count, run):
            mode = owner * own_count + start
            x_mode = mode // KY
            x_cos, x_sin = x_wave[0, pl.ds(x_mode, 1), :], x_wave[1, pl.ds(x_mode, 1), :]
            if run == KY:
                y_cos, y_sin = y_wave[0], y_wave[1]
            else:
                y_cos, y_sin = y_wave[0, :run], y_wave[1, :run]
                for other in range(run, KY, run):
                    here = mode % KY == other
                    y_cos = jnp.where(here, y_wave[0, other : other + run], y_cos)
                    y_sin = jnp.where(here, y_wave[1, other : other + run], y_sin)
            cosines.append(x_cos * y_cos - x_sin * y_sin)
            sines.append(-(x_sin * y_cos + x_cos * y_sin))
        pending += cosines + sines
        count = sum(piece.shape[0] for piece in pending)
        if count % 16 == 0:
            basis[row : row + count, :] = jnp.concatenate(pending, axis=0).astype(jnp.bfloat16)
            pending, row = [], row + count


def basis_kernel(offsets, own_count, shape, basis, x_wave, y_wave):
    write_basis(offsets, own_count, shape, x_wave, y_wave, basis)


def forward_kernel(half, basis, field, out):
    rows = out.shape[1]
    for b in range(field.shape[0]):
        product = jnp.dot(basis[half * rows : (half + 1) * rows, :], field[b], preferred_element_type=jnp.float32)
        out[b] = product.astype(out.dtype)


def skip_kernel(offsets, own_count, shape, field, skip_weight, skip, turned, x_wave, y_wave, basis):
    for b in range(field.shape[0]):
        skip[b] = jnp.dot(field[b], skip_weight[...], preferred_element_type=jnp.float32)
    write_basis(offsets, own_count, shape, x_wave, y_wave, basis)
    turned[...] = basis[...].T


def mix_kernel(scale, own_count, total, other, weight, mixed):
    micro_count, rows, width_count = total.shape
    spectrum = ((total[...] + other[...].astype(jnp.float32)) * scale).reshape(micro_count * rows, width_count)
    mode = remainder(lax.broadcasted_iota(jnp.int32, spectrum.shape, 0), own_count)
    apart = [jnp.where(mode == at, spectrum, 0.0).astype(jnp.bfloat16) for at in range(own_count)]
    apart = jnp.concatenate(apart, axis=1)
    part_width = mixed.shape[-1]
    by = []
    for kind in (0, 1):
        columns = weight[:, kind].reshape(own_count * width_count, part_width)
        product = jnp.dot(apart, columns, preferred_element_type=jnp.float32)
        by.append(product.reshape(micro_count, rows, part_width))
    real = by[0][:, :own_count] - by[1][:, own_count:]
    imaginary = by[1][:, :own_count] + by[0][:, own_count:]
    mixed[...] = jnp.concatenate([real, imaginary], axis=1).astype(jnp.bfloat16)


def gelu(value):
    inner = value * (math.sqrt(2.0 / math.pi) + (math.sqrt(2.0 / math.pi) * 0.044715) * (value * value))
    half = 0.5 * value
    return half + half * jnp.tanh(inner)


def output_kernel(
    scale, tile, chunk, y_devices, chip, mine, theirs, skip, turned, inner_weight, outer_weight, out, modes
):
    micro_count, cells, _ = skip.shape
    step = pl.program_id(0)
    tiles = cells // tile

    @pl.when(step == 0)
    def _():
        if y_devices == 1:
            count = chip.shape[2]
            for at in range(chip.shape[0]):
                for b in range(micro_count):
                    modes[b, 0, at * count : (at + 1) * count, :] = chip[at, b]
            return
        core, y_me = lax.axis_index("gx") & 1, lax.axis_index("gy")
        _, held_count, _, rows, part_width = chip.shape
        count = held_count * rows
        for b in range(micro_count):
            found = find_blocks(
                y_devices, core, lambda i: chip[i, :, b], lambda i: mine[i, :, b], lambda i: theirs[i, :, b]
            )
            for (holder, y, part), blocks in found.items():
                at = (2 * holder + y) * count
                modes[b, y_me ^ part, at : at + count, :] = blocks.reshape(count, part_width)

    b, start = step // tiles, pl.multiple_of((step % tiles) * tile, tile)
    waves = turned[pl.ds(start, tile), :]
    spectral = jnp.concatenate(
        [jnp.dot(waves, modes[b, part], preferred_element_type=jnp.float32) for part in range(modes.shape[1])], axis=1
    )
    active = gelu(spectral * scale + skip[b, pl.ds(start, tile), :]).astype(jnp.bfloat16)

    def inner(at):
        columns = inner_weight[at * chunk : (at + 1) * chunk, :]
        return lax.dot_general(active, columns, (((1,), (1,)), ((), ())), preferred_element_type=jnp.float32)

    chunks = inner_weight.shape[0] // chunk
    total, following = active.astype(jnp.float32), inner(0)
    for at in range(chunks):
        hidden = following
        if at + 1 < chunks:
            following = inner(at + 1)
        rows = outer_weight[at * chunk : (at + 1) * chunk, :]
        total = total + jnp.dot(gelu(hidden).astype(jnp.bfloat16), rows, preferred_element_type=jnp.float32)
    out[0] = total.astype(jnp.bfloat16)


def local(grid_field, spectral_weight, skip_weight, inner_weight, outer_weight):
    micro_count, row_count, col_count, width_count = grid_field.shape
    x_devices = lax.axis_size("gx")
    y_devices = lax.axis_size("gy")
    total_rows = row_count * x_devices
    total_cols = col_count * y_devices
    mode_count = KX * KY
    own_count = mode_count // x_devices
    cells = row_count * col_count
    shape = (row_count, col_count, total_rows, total_cols)
    flat_rows = grid_field.reshape(micro_count, cells, width_count)
    waves = [pltpu.VMEM((2, KX, cells), jnp.float32), pltpu.VMEM((2, KY, cells), jnp.float32)]
    basis_shape = (2 * mode_count, cells)
    matmul = 2 * micro_count * cells * width_count

    basis = pl.pallas_call(
        functools.partial(basis_kernel, reduce_offsets(x_devices), own_count, shape),
        out_shape=jax.ShapeDtypeStruct(basis_shape, jnp.bfloat16),
        out_specs=VMEM,
        scratch_shapes=waves,
        compiler_params=pltpu.CompilerParams(vmem_limit_bytes=16 * 2**20),
        cost_estimate=pl.CostEstimate(flops=8 * matmul * 2 * mode_count, bytes_accessed=2 * flat_rows.size, transcendentals=0),
        name="basis",
    )()

    def forward(half, kind):
        return pl.pallas_call(
            functools.partial(forward_kernel, half),
            out_shape=jax.ShapeDtypeStruct((micro_count, mode_count, width_count), kind),
            in_specs=[VMEM, VMEM],
            out_specs=VMEM,
            compiler_params=pltpu.CompilerParams(vmem_limit_bytes=16 * 2**20),
            cost_estimate=pl.CostEstimate(
                flops=8 * matmul * mode_count, bytes_accessed=2 * flat_rows.size, transcendentals=0
            ),
            name="forward",
        )(basis, flat_rows)

    send = forward(1, jnp.bfloat16)
    keep = forward(0, jnp.float32)

    skip, turned = pl.pallas_call(
        functools.partial(skip_kernel, gather_offsets(x_devices), own_count, shape),
        out_shape=[
            jax.ShapeDtypeStruct((micro_count, cells, width_count), jnp.float32),
            jax.ShapeDtypeStruct((cells, 2 * mode_count), jnp.bfloat16),
        ],
        in_specs=[VMEM, VMEM],
        out_specs=[VMEM, VMEM],
        scratch_shapes=waves + [pltpu.VMEM(basis_shape, jnp.bfloat16)],
        compiler_params=pltpu.CompilerParams(vmem_limit_bytes=16 * 2**20),
        cost_estimate=pl.CostEstimate(flops=matmul * width_count, bytes_accessed=2 * flat_rows.size, transcendentals=0),
        name="skip",
    )(flat_rows, skip_weight)

    def as_blocks(array):
        return array.reshape(micro_count, x_devices // 2, 2 * own_count, width_count)

    pairs, shared = reduce_peers(x_devices // 2)
    sent = exchange(send, (1, 1))
    blocks = as_blocks(keep) + as_blocks(sent).astype(jnp.float32)
    arrived = []
    for at, pair in enumerate(pairs):
        arrived.append(exchange(blocks[:, 2 * at : 2 * at + 2].astype(jnp.bfloat16), (2 * pair[0], 2 * pair[1])))
    shared_arrived = exchange(blocks[:, -2].astype(jnp.bfloat16), (2 * shared, 2 * shared))
    summed = sum(piece.astype(jnp.float32) for piece in arrived)
    swapped = exchange(summed[:, 1].astype(jnp.bfloat16), (1, 1))
    total = blocks[:, -1] + summed[:, 0] + shared_arrived.astype(jnp.float32) + swapped.astype(jnp.float32)
    for bit in range(y_devices.bit_length() - 1):
        if bit > 0:
            total = total + other.astype(jnp.float32)
        other = exchange(total.astype(jnp.bfloat16), (0, 0), (1 << bit, 1 << bit))

    part_width = spectral_weight.shape[-1]
    mixed = pl.pallas_call(
        functools.partial(mix_kernel, 1.0 / math.sqrt(total_rows * total_cols), own_count),
        out_shape=jax.ShapeDtypeStruct((micro_count, 2 * own_count, part_width), jnp.bfloat16),
        in_specs=[VMEM] * 3,
        out_specs=VMEM,
        compiler_params=pltpu.CompilerParams(vmem_limit_bytes=16 * 2**20),
        cost_estimate=pl.CostEstimate(flops=8 * spectral_weight.size, bytes_accessed=2 * spectral_weight.size, transcendentals=0),
        name="mix",
    )(total, other, spectral_weight)[None]

    pairs, shared = along_peers(x_devices // 4)
    sibling = exchange(mixed, (1, 1))
    shared_along = exchange(mixed, (4 * shared, 4 * shared))
    chip = jnp.concatenate([mixed, sibling])
    along = []
    for pair in pairs:
        along.append(exchange(chip, (4 * pair[0], 4 * pair[1])))
    held = jnp.concatenate([mixed, shared_along] + along)

    pairs, shared = plane_peers(y_devices)
    sibling = exchange(held, (1, 1))
    shared_plane = exchange(held, (2 * shared[0], 2 * shared[0]), (shared[1], shared[1]))
    chip = jnp.stack([held, sibling])
    planes = []
    for one, two in pairs:
        planes.append(exchange(chip, (2 * one[0], 2 * two[0]), (one[1], two[1])))
    shared_theirs = exchange(shared_plane, (1, 1))
    mine = jnp.concatenate(planes)
    theirs = jnp.concatenate([shared_theirs[None], exchange(mine, (1, 1))])
    mine = jnp.concatenate([shared_plane[None], mine])

    rows = 2 * own_count
    parts = y_devices
    if rows % 16 or part_width % 128:
        core = lax.axis_index("gx") & 1
        found = find_blocks(y_devices, core, lambda i: chip[i], lambda i: mine[i], lambda i: theirs[i])
        whole = jnp.stack([jnp.stack([found[h, y, p] for p in range(y_devices)]) for h in (0, 1) for y in (0, 1)])
        whole = jnp.take(whole, lax.axis_index("gy") ^ jnp.arange(y_devices, dtype=jnp.int32), axis=1)
        chip = whole.transpose(0, 3, 2, 4, 1, 5).reshape(4, micro_count, -1, width_count)
        parts, mine, theirs = 1, chip[:, :1, :16], chip[:, :1, :16]
    tile = cells
    layer_out = pl.pallas_call(
        functools.partial(output_kernel, 1.0 / math.sqrt(mode_count), tile, inner_weight.shape[0] // 2, parts),
        out_shape=jax.ShapeDtypeStruct((micro_count, cells, width_count), jnp.bfloat16),
        grid=(micro_count * cells // tile,),
        in_specs=[VMEM] * 7,
        out_specs=pl.BlockSpec((1, tile, width_count), lambda i: (i // (cells // tile), i % (cells // tile), 0)),
        scratch_shapes=[
            pltpu.VMEM((micro_count, parts, 2 * mode_count, width_count // parts), jnp.bfloat16),
        ],
        compiler_params=pltpu.CompilerParams(vmem_limit_bytes=32 * 2**20),
        cost_estimate=pl.CostEstimate(
            flops=matmul * (2 * mode_count + 2 * inner_weight.shape[0]), bytes_accessed=4 * flat_rows.size, transcendentals=0
        ),
        name="output",
    )(chip, mine, theirs, skip, turned, inner_weight, outer_weight)
    return layer_out.reshape(micro_count, row_count, col_count, width_count)


def solution(mesh):
    in_specs = (P(None, "gx", "gy", None), P("gx", None, None, "gy"), P(), P(), P())
    out_specs = P(None, "gx", "gy", None)
    return jax.shard_map(local, mesh=mesh, in_specs=in_specs, out_specs=out_specs, check_vma=False)
```
